32 devices in a mesh: tp: 8 (over y, x, core), col: 4 (over z).
Axes of the slice: x: 2, y: 2, z: 4, core: 2. Of those that a mesh axis runs over, the one named last changes fastest.
Arguments:
- gate_in: bfloat16 [128, 53248], P('col', 'tp'), may hold values from -6 to 6
- up_in: bfloat16 [128, 53248], P('col', 'tp'), may hold values from -6 to 6
- down_weight: bfloat16 [53248, 16384], P('tp', 'col'), may hold values from -0.02734375 to 0.02734375
- residual: bfloat16 [128, 16384], P('tp', 'col'), may hold values from -30 to 30
- norm_gain: bfloat16 [16384], P('col'), may hold values from 0.5 to 1.5
Outputs:
- stream: bfloat16 [128, 16384], P('tp', 'col')
- normed: bfloat16 [128, 16384], P('tp', 'col')
The draws below stay inside these ranges and needn't reach their ends.
All inputs are finite; a program needn't handle non-finite values.
Results may differ from the reference program's by a relative error of at most 0.0034.
Values may be sent and summed in bfloat16 or wider, within the bound.
A program may use at most 128 MiB of HBM per device.

```python
import math
import jax
import jax.numpy as jnp
from jax import lax

D = 16384
FF = 53248
TOKENS = 128


def draw_residual(key, part):
    key_rows = jax.random.fold_in(key, 11)
    key_values = jax.random.fold_in(key, 23)
    row_scale = jnp.exp(jax.random.uniform(key_rows, (TOKENS, 1), jnp.float32, math.log(0.3), math.log(3.0)))
    ramp = jnp.arange(D, dtype=jnp.float32) / (D - 1)
    col_scale = 0.5 * jnp.exp(ramp * math.log(3.0))
    values = jnp.clip(jax.random.normal(key_values, (TOKENS, D), jnp.float32), -4.0, 4.0)
    return (row_scale * col_scale[None, :] * values).astype(jnp.bfloat16)


def levels(stream_key, extent, shards, smallest, high):
    def one(position, parts):
        draws = jax.random.uniform(jax.random.fold_in(jax.random.fold_in(stream_key, 6), position), (parts,), jnp.float32, smallest / len(shards), high / len(shards))
        return jnp.repeat(jnp.exp(draws), extent[position] // parts).reshape((-1,) + (1,) * (len(extent) - position - 1))

    factor_of = one(*shards[0])
    for cut in shards[1:]:
        factor_of = factor_of * one(*cut)
    return factor_of


def noise(key, dims, scale, most, cuts=(), kind=jnp.bfloat16):
    drawn = scale * jax.random.normal(key, dims, jnp.float32)
    if cuts:
        drawn = drawn * levels(key, dims, cuts, -0.22, 0.18)
    return jnp.clip(drawn, -most, most).astype(kind)


def setup_inputs(seed: int = 0) -> dict:
    arg_keys = jax.random.split(jax.random.key(seed), 6)
    return {
        "gate_in": noise(arg_keys[0], (TOKENS, FF), 1.0, 6.0, ((0, 4), (1, 8))),
        "up_in": noise(arg_keys[1], (TOKENS, FF), 1.0, 6.0, ((0, 4), (1, 8))),
        "down_weight": noise(arg_keys[2], (FF, D), FF ** -0.5, 0.02734375, ((0, 8), (1, 4))),
        "residual": draw_residual(jax.random.fold_in(arg_keys[5], 71), 0),
        "norm_gain": jnp.clip(1.0 + 0.1 * jax.random.normal(arg_keys[4], (D,), jnp.float32), 0.5, 1.5).astype(jnp.bfloat16),
    }


def reference(gate_in, up_in, down_weight, residual, norm_gain):
    hidden = (jax.nn.silu(gate_in.astype(jnp.float32)) * up_in.astype(jnp.float32)).astype(jnp.bfloat16)
    branch = jnp.dot(hidden, down_weight, preferred_element_type=jnp.float32)
    summed = residual.astype(jnp.float32) + branch
    mean_square = lax.optimization_barrier(jnp.mean(summed * summed, axis=1, keepdims=True))
    scaled = summed * lax.rsqrt(mean_square + 1e-05) * norm_gain.astype(jnp.float32)[None, :]
    return (summed.astype(jnp.bfloat16), scaled.astype(jnp.bfloat16))
```

```python
import functools

import jax
import jax.numpy as jnp
from jax import lax
from jax.experimental import pallas as pl
from jax.experimental.pallas import tpu as pltpu
from jax.sharding import PartitionSpec as P

MESH = pl.DeviceIdType.MESH
VMEM_BYTES = 67_043_328
EPS = 1e-05
SKEW = 5
SPLIT = 5


def gated(gate_part, up_part):
    return (jax.nn.silu(gate_part.astype(jnp.float32)) * up_part.astype(jnp.float32)).astype(
        jnp.bfloat16
    )


def plain_body(width, gate_in, up_in, down_weight, residual, norm_gain):
    local_act = gated(gate_in, up_in)
    hidden = lax.all_gather(local_act, "col", axis=0, tiled=True)
    partial_value = jnp.dot(hidden, down_weight, preferred_element_type=jnp.float32)
    branch = lax.psum_scatter(partial_value, "tp", scatter_dimension=0, tiled=True)
    summed = residual.astype(jnp.float32) + branch
    local_squares = jnp.sum(summed * summed, axis=1, keepdims=True)
    mean_square = lax.psum(local_squares, "col") / width
    scaled = summed * lax.rsqrt(mean_square + EPS) * norm_gain.astype(jnp.float32)[None, :]
    return (summed.astype(jnp.bfloat16), scaled.astype(jnp.bfloat16))


def pick(extent, most, step):
    best = 0
    for size in range(step, min(extent, most) + 1, step):
        if extent % size == 0:
            best = size
    return best


def kernel(
    n_col, n_pair, kp, nt, rt, skew, split, width_all,
    gate_hbm, up_hbm, w_hbm, res_hbm, gain_hbm,
    total_hbm, pre_hbm, scale_out,
    gate_v, up_v, hid, w_v, acc, peer, send_buf, recv_buf, total, pre, res_v, gain_v, squares,
    in_sem, w_sem, res_sem, gain_sem, out_sem,
    ag_send, ag_recv, d_send, d_recv, r_send, r_recv, q_send, q_recv,
):
    depth = gate_hbm.shape[1]
    width = w_hbm.shape[1]
    half = res_hbm.shape[0]
    pieces = depth // kp
    whole_units = pieces - split
    units = pieces + split
    tiles = width // rt
    me = lax.axis_index("tp")
    z = lax.axis_index("col")
    plane, core = me // 2, lax.rem(me, 2)

    barrier = pltpu.get_barrier_semaphore()
    for step in range(1, n_col):
        pl.semaphore_signal(
            barrier, inc=1, device_id={"col": lax.rem(z + step, n_col)}, device_id_type=MESH
        )
    pl.semaphore_signal(barrier, inc=1, device_id={"tp": 2 * plane + 1 - core}, device_id_type=MESH)
    for step in range(1, n_pair):
        pl.semaphore_signal(
            barrier,
            inc=1,
            device_id={"tp": 2 * lax.rem(plane + step, n_pair) + core},
            device_id_type=MESH,
        )

    def cols(s):
        return pl.ds(pl.multiple_of(s * kp, kp), kp)

    def load(s, which):
        src, dst = ((gate_hbm, gate_v), (up_hbm, up_v))[which]
        return pltpu.make_async_copy(src.at[:, cols(s)], dst.at[:, cols(s)], in_sem.at[which, s])

    def load_w(s):
        return pltpu.make_async_copy(w_hbm.at[cols(s), :], w_v.at[cols(s), :], w_sem.at[s])

    load_res = pltpu.make_async_copy(res_hbm, res_v, res_sem)
    load_gain = pltpu.make_async_copy(gain_hbm, gain_v, gain_sem)

    @pl.loop(0, pieces)
    def _(s):
        load(s, 0).start()
        load(s, 1).start()

    @pl.loop(0, pieces)
    def _(s):
        load_w(s).start()

    load_res.start()
    load_gain.start()

    def source_rows(source):
        return pl.ds(pl.multiple_of(source * half, half), half)

    def hop(source, group, s, to):
        block = hid.at[group, source_rows(source), cols(s)]
        return pltpu.make_async_remote_copy(
            src_ref=block,
            dst_ref=block,
            send_sem=ag_send.at[(1 + to) // 2, source],
            recv_sem=ag_recv.at[source, group, s],
            device_id={"col": z + to},
            device_id_type=MESH,
        )

    def unit(u):
        group = (u >= pieces).astype(jnp.int32)
        return group, u - split * group

    def each(source, u, to, action):
        group, s = unit(u)
        action(hop(source, group, s, to))

        @pl.when(u < whole_units)
        def _():
            action(hop(source, 1, s, to))

    def start(copy):
        copy.start()

    def pass_on(source, u, to, forward):
        each(source, u, to, lambda copy: copy.wait_recv())

        @pl.when(forward)
        def _():
            each(source, u, to, start)

    below, above = z, n_col - 1 - z
    few, many = jnp.minimum(below, above), jnp.maximum(below, above)
    inward = jnp.where(below < above, 1, -1)
    lag = skew * jnp.maximum(many - 1, 0)
    lead = jnp.where(few > 0, skew, pieces)

    pl.semaphore_wait(barrier, n_col - 1 + 1 + n_pair - 1)

    @pl.loop(0, pieces + 1)
    def _(s):
        @pl.when(s < pieces)
        def _():
            load(s, 0).wait()
            load(s, 1).wait()
            g = gate_v[:, cols(s)].astype(jnp.float32)
            u = up_v[:, cols(s)].astype(jnp.float32)
            h = (g / (1.0 + jnp.exp(-g)) * u).astype(jnp.bfloat16)
            hid[0, source_rows(z), cols(s)] = h[:half]
            hid[1, source_rows(z), cols(s)] = h[half:]

        @pl.when(s > 0)
        def _():
            u = s - 1

            @pl.when(u < lead)
            def _():
                each(z, u, inward, start)

            @pl.when(few > 0)
            def _():
                each(z, u, -inward, start)

    acc[...] = jnp.zeros_like(acc)

    def swap(group, n):
        here = pl.ds(n * rt, rt)
        return pltpu.make_async_remote_copy(
            src_ref=acc.at[group, :, :, here],
            dst_ref=peer.at[:, :, here],
            send_sem=d_send,
            recv_sem=d_recv.at[n],
            device_id={"tp": 2 * plane + 1 - core},
            device_id_type=MESH,
        )

    def scatter(n, step):
        to = lax.rem(plane + step, n_pair)
        here = pl.ds(n * rt, rt)
        return pltpu.make_async_remote_copy(
            src_ref=send_buf.at[to, :, here],
            dst_ref=recv_buf.at[step - 1, :, here],
            send_sem=r_send.at[step - 1],
            recv_sem=r_recv.at[step - 1, n],
            device_id={"tp": 2 * to + core},
            device_id_type=MESH,
        )

    def sum_pair(group):
        for n in range(tiles + 1):
            if n < tiles:
                here = slice(n * rt, (n + 1) * rt)
                swap(group, n).wait_recv()
                send_buf[:, :, here] = (acc[group, :, :, here] + peer[:, :, here]).astype(
                    jnp.bfloat16
                )
                total[:, here] = (
                    acc[group, plane, :, here]
                    + peer[plane, :, here]
                    + res_v[:, here].astype(jnp.float32)
                )
            if n > 0:
                for step in range(1, n_pair):
                    scatter(n - 1, step).start()

    @pl.loop(0, units + skew * (n_col - 2))
    def _(i):
        for away in range(1, (n_col + 1) // 2):

            @pl.when(jnp.logical_and(few >= away, i < units))
            def _():
                pass_on(z - inward * away, i, inward, True)

        mine = i + lead

        @pl.when(mine < units)
        def _():
            each(z, mine, inward, start)

        u = i - lag
        live = jnp.logical_and(u >= 0, u < units)
        for away in range(1, n_col):

            @pl.when(jnp.logical_and(live, many >= away))
            def _():
                pass_on(z + inward * away, u, -inward, few > 0)

        @pl.when(jnp.logical_and(jnp.logical_and(u >= pieces, u < units), few > 0))
        def _():
            each(z, u, -inward, start)

        @pl.when(jnp.logical_and(u == pieces, core == 1))
        def _():
            for n in range(tiles):
                swap(0, n).start()

        @pl.when(jnp.logical_and(u >= 0, u < pieces))
        def _():
            load_w(u).wait()

        @pl.when(jnp.logical_and(u >= 0, u < whole_units))
        def _():
            a = hid[:, :, cols(u)].reshape(2 * n_col * half, kp)
            for n in range(width // nt):
                here = slice(n * nt, (n + 1) * nt)
                part = jnp.dot(a, w_v[cols(u), here], preferred_element_type=jnp.float32)
                acc[:, :, :, here] += part.reshape(2, n_pair, half, nt)

        @pl.when(jnp.logical_and(u >= whole_units, u < units - 1))
        def _():
            group, s = unit(u)
            a = hid[group, :, cols(s)]
            for n in range(width // nt):
                here = slice(n * nt, (n + 1) * nt)
                part = jnp.dot(a, w_v[cols(s), here], preferred_element_type=jnp.float32)
                acc[group, :, :, here] += part.reshape(n_pair, half, nt)

        @pl.when(jnp.logical_and(u == pieces + split // 2 + 1, core == 0))
        def _():
            load_res.wait()
            load_gain.wait()
            sum_pair(0)

    last = pl.ds((pieces - 1) * kp, kp)
    a = hid[1, :, last]
    for n in range(tiles + 1):
        if n < tiles:
            here = slice(n * rt, (n + 1) * rt)
            part = jnp.dot(a, w_v[last, here], preferred_element_type=jnp.float32)
            acc[1, :, :, here] += part.reshape(n_pair, half, rt)
        if n > 0:

            @pl.when(core == 0)
            def _():
                swap(1, n - 1).start()

    @pl.when(core == 1)
    def _():
        load_res.wait()
        load_gain.wait()
        sum_pair(1)

    sums = jnp.zeros((half, 128), jnp.float32)
    gain = gain_v[...].astype(jnp.float32)
    writes = []
    for n in range(tiles):
        here = slice(n * rt, (n + 1) * rt)
        value = total[:, here]
        for step in range(1, n_pair):
            scatter(n, step).wait_recv()
            value = value + recv_buf[step - 1, :, here].astype(jnp.float32)
        total[:, here] = value
        square = value * value
        for j in range(rt // 128):
            lane = n * (rt // 128) + j
            sums = sums + square[:, j * 128 : (j + 1) * 128]
            pre[:, lane * 128 : (lane + 1) * 128] = (
                value[:, j * 128 : (j + 1) * 128] * gain[lane : lane + 1, :]
            )
        if n == tiles - 1:
            squares[z] = jnp.broadcast_to(jnp.sum(sums, axis=1, keepdims=True), sums.shape)

    def share(step):
        return pltpu.make_async_remote_copy(
            src_ref=squares.at[z],
            dst_ref=squares.at[z],
            send_sem=q_send.at[step - 1],
            recv_sem=q_recv.at[step - 1],
            device_id={"col": lax.rem(z + step, n_col)},
            device_id_type=MESH,
        )

    def arrival(step):
        block = squares.at[lax.rem(z + n_col - step, n_col)]
        return pltpu.make_async_remote_copy(
            src_ref=block,
            dst_ref=block,
            send_sem=q_send.at[step - 1],
            recv_sem=q_recv.at[step - 1],
            device_id={"col": lax.rem(z + step, n_col)},
            device_id_type=MESH,
        )

    for step in range(1, n_col):
        share(step).start()
    writes = [
        pltpu.make_async_copy(total, total_hbm, out_sem.at[0]),
        pltpu.make_async_copy(pre, pre_hbm, out_sem.at[1]),
    ]
    for write in writes:
        write.start()

    for source in range(n_col):
        block = hid.at[:, source * half : (source + 1) * half, :]
        for up in (0, 1):
            sent = jnp.logical_and(source >= z, z > 0)
            if up:
                sent = jnp.logical_and(source <= z, z < n_col - 1)

            @pl.when(sent)
            def _():
                pltpu.make_async_remote_copy(
                    src_ref=block,
                    dst_ref=block,
                    send_sem=ag_send.at[up, source],
                    recv_sem=ag_recv.at[source, 0, 0],
                    device_id={"col": z + 1 if up else z - 1},
                    device_id_type=MESH,
                ).wait_send()

    pltpu.make_async_remote_copy(
        src_ref=peer,
        dst_ref=peer,
        send_sem=d_send,
        recv_sem=d_recv.at[0],
        device_id={"tp": 2 * plane + 1 - core},
        device_id_type=MESH,
    ).wait_send()
    for step in range(1, n_pair):
        to = lax.rem(plane + step, n_pair)
        pltpu.make_async_remote_copy(
            src_ref=send_buf.at[to],
            dst_ref=recv_buf.at[step - 1],
            send_sem=r_send.at[step - 1],
            recv_sem=r_recv.at[step - 1, 0],
            device_id={"tp": 2 * to + core},
            device_id_type=MESH,
        ).wait_send()
    for write in writes:
        write.wait()
    for step in range(1, n_col):
        share(step).wait_send()
        arrival(step).wait_recv()
    whole = squares[0]
    for j in range(1, n_col):
        whole = whole + squares[j]
    scale_out[...] = lax.rsqrt(whole / width_all + EPS)


def finish(total_ref, pre_ref, scale_ref, stream_ref, normed_ref):
    stream_ref[...] = total_ref[...].astype(jnp.bfloat16)
    scale = scale_ref[...]
    for j in range(total_ref.shape[1] // 128):
        here = slice(j * 128, (j + 1) * 128)
        normed_ref[:, here] = (pre_ref[:, here] * scale).astype(jnp.bfloat16)


def fused_body(n_tp, n_col, kp, nt, rt, width, gate_in, up_in, down_weight, residual, norm_gain):
    rows, depth = gate_in.shape
    local = down_weight.shape[1]
    half = residual.shape[0]
    n_pair = n_tp // 2
    pieces, tiles = depth // kp, local // rt
    any_space = pl.BlockSpec(memory_space=pl.ANY)
    vmem = pl.BlockSpec(memory_space=pltpu.VMEM)
    dma = pltpu.SemaphoreType.DMA
    block32 = jax.ShapeDtypeStruct((half, local), jnp.float32)
    total, pre, scale = pl.pallas_call(
        functools.partial(kernel, n_col, n_pair, kp, nt, rt, SKEW, SPLIT, width),
        out_shape=(block32, block32, jax.ShapeDtypeStruct((half, 128), jnp.float32)),
        in_specs=[any_space] * 5,
        out_specs=(any_space, any_space, vmem),
        scratch_shapes=[
            pltpu.VMEM((rows, depth), jnp.bfloat16),
            pltpu.VMEM((rows, depth), jnp.bfloat16),
            pltpu.VMEM((2, half * n_col, depth), jnp.bfloat16),
            pltpu.VMEM((depth, local), jnp.bfloat16),
            pltpu.VMEM((2, n_pair, half, local), jnp.float32),
            pltpu.VMEM((n_pair, half, local), jnp.float32),
            pltpu.VMEM((n_pair, half, local), jnp.bfloat16),
            pltpu.VMEM((n_pair - 1, half, local), jnp.bfloat16),
            pltpu.VMEM((half, local), jnp.float32),
            pltpu.VMEM((half, local), jnp.float32),
            pltpu.VMEM((half, local), jnp.bfloat16),
            pltpu.VMEM((local // 128, 128), jnp.bfloat16),
            pltpu.VMEM((n_col, half, 128), jnp.float32),
            dma((2, pieces)),
            dma((pieces,)),
            dma,
            dma,
            dma((2,)),
            dma((2, n_col)),
            dma((n_col, 2, pieces)),
            dma,
            dma((tiles,)),
            dma((n_pair - 1,)),
            dma((n_pair - 1, tiles)),
            dma((n_col - 1,)),
            dma((n_col - 1,)),
        ],
        compiler_params=pltpu.CompilerParams(
            collective_id=0, has_side_effects=True, vmem_limit_bytes=VMEM_BYTES
        ),
        name="down_reduce",
    )(gate_in, up_in, down_weight, residual, norm_gain.reshape(-1, 128))
    out = jax.ShapeDtypeStruct((half, local), jnp.bfloat16)
    return pl.pallas_call(
        finish, out_shape=(out, out), in_specs=[vmem] * 3, out_specs=(vmem, vmem), name="finish"
    )(total, pre, scale)


def pairs_share_chip(mesh):
    if tuple(mesh.axis_names) != ("tp", "col") or mesh.shape["tp"] % 2 or mesh.shape["tp"] < 4:
        return False
    devices = mesh.devices
    for j in range(0, mesh.shape["tp"], 2):
        for a, b in zip(devices[j], devices[j + 1]):
            first = getattr(a, "coords", None)
            if first is None or list(first) != list(getattr(b, "coords", ())):
                return False
    return True


def solution(mesh):
    in_specs = (P("col", "tp"), P("col", "tp"), P("tp", "col"), P("tp", "col"), P("col"))
    out_specs = (P("tp", "col"), P("tp", "col"))
    n_tp, n_col = mesh.shape["tp"], mesh.shape["col"]

    def run(gate_in, up_in, down_weight, residual, norm_gain):
        tokens, hidden_units = gate_in.shape
        width = down_weight.shape[1]
        depth, local = hidden_units // n_tp, width // n_col
        rows, own_rows = tokens // n_col, tokens // n_tp
        kp, nt, rt = pick(depth, 512, 128), pick(local, 1024, 128), pick(local, 512, 128)
        need = 2 * depth * (local + tokens + 2 * rows) + local * tokens * 9 + (4 << 20)
        fused = (
            pairs_share_chip(mesh)
            and n_col > 1
            and rows % 16 == 0
            and own_rows % 16 == 0
            and rows == 2 * own_rows
            and n_tp == 2 * n_col
            and local % 1024 == 0
            and kp > 0
            and SKEW < SPLIT + 1 < depth // kp
            and nt > 0
            and need < VMEM_BYTES
        )
        body = functools.partial(plain_body, width)
        if fused:
            body = functools.partial(fused_body, n_tp, n_col, kp, nt, rt, width)
        return jax.shard_map(
            body, mesh=mesh, in_specs=in_specs, out_specs=out_specs, check_vma=False
        )(gate_in, up_in, down_weight, residual, norm_gain)

    return run
```

```python
import functools

import jax
import jax.numpy as jnp
from jax import lax
from jax.experimental import pallas as pl
from jax.experimental.pallas import tpu as pltpu
from jax.sharding import PartitionSpec as P

MESH = pl.DeviceIdType.MESH
VMEM_BYTES = 67_043_328
EPS = 1e-05
SKEW = 4
SPLIT = 5


def gated(gate_part, up_part):
    return (jax.nn.silu(gate_part.astype(jnp.float32)) * up_part.astype(jnp.float32)).astype(
        jnp.bfloat16
    )


def plain_body(width, gate_in, up_in, down_weight, residual, norm_gain):
    local_act = gated(gate_in, up_in)
    hidden = lax.all_gather(local_act, "col", axis=0, tiled=True)
    partial_value = jnp.dot(hidden, down_weight, preferred_element_type=jnp.float32)
    branch = lax.psum_scatter(partial_value, "tp", scatter_dimension=0, tiled=True)
    summed = residual.astype(jnp.float32) + branch
    local_squares = jnp.sum(summed * summed, axis=1, keepdims=True)
    mean_square = lax.psum(local_squares, "col") / width
    scaled = summed * lax.rsqrt(mean_square + EPS) * norm_gain.astype(jnp.float32)[None, :]
    return (summed.astype(jnp.bfloat16), scaled.astype(jnp.bfloat16))


def pick(extent, most, step):
    best = 0
    for size in range(step, min(extent, most) + 1, step):
        if extent % size == 0:
            best = size
    return best


def kernel(
    n_col, n_pair, kp, nt, rt, skew, split, width_all,
    gate_hbm, up_hbm, w_hbm, res_hbm, gain_hbm,
    total_hbm, pre_hbm, scale_out,
    gate_v, up_v, hid, w_v, acc, peer, send_buf, recv_buf, total, pre, res_v, gain_v, squares,
    in_sem, w_sem, res_sem, gain_sem, out_sem,
    ag_send, ag_recv, d_send, d_recv, r_send, r_recv, q_send, q_recv, ready,
):
    depth = gate_hbm.shape[1]
    width = w_hbm.shape[1]
    half = res_hbm.shape[0]
    pieces = depth // kp
    whole_units = pieces - split
    units = pieces + split
    tiles = width // rt
    me = lax.axis_index("tp")
    z = lax.axis_index("col")
    plane, core = me // 2, lax.rem(me, 2)

    below, above = z, n_col - 1 - z
    few, many = jnp.minimum(below, above), jnp.maximum(below, above)
    inward = jnp.where(below < above, 1, -1)
    far_step = lax.rem(2 * n_pair - 1 - 2 * plane, n_pair)
    beside = {"tp": 2 * plane + 1 - core}

    def chip(step):
        return {"tp": 2 * lax.rem(plane + step, n_pair) + core}

    def tell(semaphore, device):
        pl.semaphore_signal(semaphore, inc=1, device_id=device, device_id_type=MESH)

    def tell_near(semaphore):
        for step in range(1, n_pair):

            @pl.when(step != far_step)
            def _():
                tell(semaphore, chip(step))

    barrier = pltpu.get_barrier_semaphore()
    tell(barrier, {"col": z + inward})

    @pl.when(few > 0)
    def _():
        tell(barrier, {"col": z - inward})

    tell_near(barrier)
    tell(barrier, beside)

    def cols(s):
        return pl.ds(pl.multiple_of(s * kp, kp), kp)

    def load(s, which):
        src, dst = ((gate_hbm, gate_v), (up_hbm, up_v))[which]
        return pltpu.make_async_copy(src.at[:, cols(s)], dst.at[:, cols(s)], in_sem.at[which, s])

    def load_w(s):
        return pltpu.make_async_copy(w_hbm.at[cols(s), :], w_v.at[cols(s), :], w_sem.at[s])

    load_res = pltpu.make_async_copy(res_hbm, res_v, res_sem)
    load_gain = pltpu.make_async_copy(gain_hbm, gain_v, gain_sem)

    @pl.loop(0, pieces)
    def _(s):
        load(s, 0).start()
        load(s, 1).start()

    @pl.loop(0, pieces)
    def _(s):
        load_w(s).start()

    load_res.start()
    load_gain.start()

    def source_rows(source):
        return pl.ds(pl.multiple_of(source * half, half), half)

    def hop(source, group, s, to):
        block = hid.at[group, source_rows(source), cols(s)]
        return pltpu.make_async_remote_copy(
            src_ref=block,
            dst_ref=block,
            send_sem=ag_send.at[(1 + to) // 2, source],
            recv_sem=ag_recv.at[source, group, s],
            device_id={"col": z + to},
            device_id_type=MESH,
        )

    def unit(u):
        group = (u >= pieces).astype(jnp.int32)
        return group, u - split * group

    def each(source, u, to, action):
        group, s = unit(u)
        action(hop(source, group, s, to))

        @pl.when(u < whole_units)
        def _():
            action(hop(source, 1, s, to))

    def start(copy):
        copy.start()

    def pass_on(source, u, to, forward):
        each(source, u, to, lambda copy: copy.wait_recv())

        @pl.when(forward)
        def _():
            each(source, u, to, start)

    lag = skew * jnp.maximum(many - 1, 0)
    lead = jnp.where(few > 0, skew, pieces)

    pl.semaphore_wait(barrier, 1 + jnp.minimum(few, 1) + n_pair - 2 + 1)
    tell_near(ready)

    @pl.loop(0, pieces + 1)
    def _(s):
        @pl.when(s < pieces)
        def _():
            load(s, 0).wait()
            load(s, 1).wait()
            g = gate_v[:, cols(s)].astype(jnp.float32)
            u = up_v[:, cols(s)].astype(jnp.float32)
            h = (g / (1.0 + jnp.exp(-g)) * u).astype(jnp.bfloat16)
            hid[0, source_rows(z), cols(s)] = h[:half]
            hid[1, source_rows(z), cols(s)] = h[half:]

        @pl.when(s > 0)
        def _():
            u = s - 1

            @pl.when(u < lead)
            def _():
                each(z, u, inward, start)

            @pl.when(few > 0)
            def _():
                each(z, u, -inward, start)

    acc[...] = jnp.zeros_like(acc)

    def swap(group, n):
        here = pl.ds(n * rt, rt)
        return pltpu.make_async_remote_copy(
            src_ref=acc.at[group, :, :, here],
            dst_ref=peer.at[:, :, here],
            send_sem=d_send,
            recv_sem=d_recv.at[n],
            device_id=beside,
            device_id_type=MESH,
        )

    def scatter(n, step):
        to = lax.rem(plane + step, n_pair)
        here = pl.ds(n * rt, rt)
        return pltpu.make_async_remote_copy(
            src_ref=send_buf.at[to, :, here],
            dst_ref=recv_buf.at[step - 1, :, here],
            send_sem=r_send.at[step - 1],
            recv_sem=r_recv.at[step - 1, n],
            device_id={"tp": 2 * to + core},
            device_id_type=MESH,
        )

    def sum_pair(group):
        load_res.wait()
        load_gain.wait()
        pl.semaphore_wait(ready, n_pair - 2)
        for n in range(tiles + 1):
            if n < tiles:
                here = slice(n * rt, (n + 1) * rt)
                swap(group, n).wait_recv()
                send_buf[:, :, here] = (acc[group, :, :, here] + peer[:, :, here]).astype(
                    jnp.bfloat16
                )
                total[:, here] = (
                    acc[group, plane, :, here]
                    + peer[plane, :, here]
                    + res_v[:, here].astype(jnp.float32)
                )
            if n > 0:
                scatter(n - 1, far_step).start()
                for step in range(1, n_pair):

                    @pl.when(step != far_step)
                    def _():
                        scatter(n - 1, step).start()

    @pl.loop(0, units + skew * (n_col - 2))
    def _(i):
        for away in range(1, (n_col + 1) // 2):

            @pl.when(jnp.logical_and(few >= away, i < units))
            def _():
                pass_on(z - inward * away, i, inward, True)

        mine = i + lead

        @pl.when(mine < units)
        def _():
            each(z, mine, inward, start)

        u = i - lag
        live = jnp.logical_and(u >= 0, u < units)
        for away in range(1, n_col):

            @pl.when(jnp.logical_and(live, many >= away))
            def _():
                pass_on(z + inward * away, u, -inward, few > 0)

        @pl.when(jnp.logical_and(jnp.logical_and(u >= pieces, u < units), few > 0))
        def _():
            each(z, u, -inward, start)

        @pl.when(jnp.logical_and(u == pieces, core == 1))
        def _():
            for n in range(tiles):
                swap(0, n).start()

        @pl.when(jnp.logical_and(u >= 0, u < pieces))
        def _():
            load_w(u).wait()

        @pl.when(jnp.logical_and(u >= 0, u < whole_units))
        def _():
            a = hid[:, :, cols(u)].reshape(2 * n_col * half, kp)
            for n in range(width // nt):
                here = slice(n * nt, (n + 1) * nt)
                part = jnp.dot(a, w_v[cols(u), here], preferred_element_type=jnp.float32)
                acc[:, :, :, here] += part.reshape(2, n_pair, half, nt)

        @pl.when(jnp.logical_and(u >= whole_units, u < units - 1))
        def _():
            group, s = unit(u)
            a = hid[group, :, cols(s)]
            for n in range(width // nt):
                here = slice(n * nt, (n + 1) * nt)
                part = jnp.dot(a, w_v[cols(s), here], preferred_element_type=jnp.float32)
                acc[group, :, :, here] += part.reshape(n_pair, half, nt)

        @pl.when(jnp.logical_and(u == pieces + split // 2, core == 0))
        def _():
            sum_pair(0)

    last = pl.ds((pieces - 1) * kp, kp)
    a = hid[1, :, last]
    for n in range(tiles + 1):
        if n < tiles:
            here = slice(n * rt, (n + 1) * rt)
            part = jnp.dot(a, w_v[last, here], preferred_element_type=jnp.float32)
            acc[1, :, :, here] += part.reshape(n_pair, half, rt)
        if n > 0:

            @pl.when(core == 0)
            def _():
                swap(1, n - 1).start()

    @pl.when(core == 1)
    def _():
        sum_pair(1)

    sums = jnp.zeros((half, 128), jnp.float32)
    gain = gain_v[...].astype(jnp.float32)
    writes = []
    for n in range(tiles):
        here = slice(n * rt, (n + 1) * rt)
        value = total[:, here]
        for step in range(1, n_pair):
            scatter(n, step).wait_recv()
            value = value + recv_buf[step - 1, :, here].astype(jnp.float32)
        total[:, here] = value
        square = value * value
        for j in range(rt // 128):
            lane = n * (rt // 128) + j
            sums = sums + square[:, j * 128 : (j + 1) * 128]
            pre[:, lane * 128 : (lane + 1) * 128] = (
                value[:, j * 128 : (j + 1) * 128] * gain[lane : lane + 1, :]
            )
        if n == tiles - 1:
            squares[z] = jnp.broadcast_to(jnp.sum(sums, axis=1, keepdims=True), sums.shape)

    def share(step):
        return pltpu.make_async_remote_copy(
            src_ref=squares.at[z],
            dst_ref=squares.at[z],
            send_sem=q_send.at[step - 1],
            recv_sem=q_recv.at[step - 1],
            device_id={"col": lax.rem(z + step, n_col)},
            device_id_type=MESH,
        )

    def arrival(step):
        block = squares.at[lax.rem(z + n_col - step, n_col)]
        return pltpu.make_async_remote_copy(
            src_ref=block,
            dst_ref=block,
            send_sem=q_send.at[step - 1],
            recv_sem=q_recv.at[step - 1],
            device_id={"col": lax.rem(z + step, n_col)},
            device_id_type=MESH,
        )

    for step in range(1, n_col):
        share(step).start()
    writes = [
        pltpu.make_async_copy(total, total_hbm, out_sem.at[0]),
        pltpu.make_async_copy(pre, pre_hbm, out_sem.at[1]),
    ]
    for write in writes:
        write.start()

    for source in range(n_col):
        block = hid.at[:, source * half : (source + 1) * half, :]
        for up in (0, 1):
            sent = jnp.logical_and(source >= z, z > 0)
            if up:
                sent = jnp.logical_and(source <= z, z < n_col - 1)

            @pl.when(sent)
            def _():
                pltpu.make_async_remote_copy(
                    src_ref=block,
                    dst_ref=block,
                    send_sem=ag_send.at[up, source],
                    recv_sem=ag_recv.at[source, 0, 0],
                    device_id={"col": z + 1 if up else z - 1},
                    device_id_type=MESH,
                ).wait_send()

    pltpu.make_async_remote_copy(
        src_ref=peer,
        dst_ref=peer,
        send_sem=d_send,
        recv_sem=d_recv.at[0],
        device_id=beside,
        device_id_type=MESH,
    ).wait_send()
    for step in range(1, n_pair):
        to = lax.rem(plane + step, n_pair)
        pltpu.make_async_remote_copy(
            src_ref=send_buf.at[to],
            dst_ref=recv_buf.at[step - 1],
            send_sem=r_send.at[step - 1],
            recv_sem=r_recv.at[step - 1, 0],
            device_id={"tp": 2 * to + core},
            device_id_type=MESH,
        ).wait_send()
    for write in writes:
        write.wait()
    for step in range(1, n_col):
        share(step).wait_send()
        arrival(step).wait_recv()
    whole = squares[0]
    for j in range(1, n_col):
        whole = whole + squares[j]
    scale_out[...] = lax.rsqrt(whole / width_all + EPS)


def finish(total_ref, pre_ref, scale_ref, stream_ref, normed_ref):
    stream_ref[...] = total_ref[...].astype(jnp.bfloat16)
    scale = scale_ref[...]
    for j in range(total_ref.shape[1] // 128):
        here = slice(j * 128, (j + 1) * 128)
        normed_ref[:, here] = (pre_ref[:, here] * scale).astype(jnp.bfloat16)


def fused_body(n_tp, n_col, kp, nt, rt, width, gate_in, up_in, down_weight, residual, norm_gain):
    rows, depth = gate_in.shape
    local = down_weight.shape[1]
    half = residual.shape[0]
    n_pair = n_tp // 2
    pieces, tiles = depth // kp, local // rt
    any_space = pl.BlockSpec(memory_space=pl.ANY)
    vmem = pl.BlockSpec(memory_space=pltpu.VMEM)
    dma = pltpu.SemaphoreType.DMA
    block32 = jax.ShapeDtypeStruct((half, local), jnp.float32)
    total, pre, scale = pl.pallas_call(
        functools.partial(kernel, n_col, n_pair, kp, nt, rt, SKEW, SPLIT, width),
        out_shape=(block32, block32, jax.ShapeDtypeStruct((half, 128), jnp.float32)),
        in_specs=[any_space] * 5,
        out_specs=(any_space, any_space, vmem),
        scratch_shapes=[
            pltpu.VMEM((rows, depth), jnp.bfloat16),
            pltpu.VMEM((rows, depth), jnp.bfloat16),
            pltpu.VMEM((2, half * n_col, depth), jnp.bfloat16),
            pltpu.VMEM((depth, local), jnp.bfloat16),
            pltpu.VMEM((2, n_pair, half, local), jnp.float32),
            pltpu.VMEM((n_pair, half, local), jnp.float32),
            pltpu.VMEM((n_pair, half, local), jnp.bfloat16),
            pltpu.VMEM((n_pair - 1, half, local), jnp.bfloat16),
            pltpu.VMEM((half, local), jnp.float32),
            pltpu.VMEM((half, local), jnp.float32),
            pltpu.VMEM((half, local), jnp.bfloat16),
            pltpu.VMEM((local // 128, 128), jnp.bfloat16),
            pltpu.VMEM((n_col, half, 128), jnp.float32),
            dma((2, pieces)),
            dma((pieces,)),
            dma,
            dma,
            dma((2,)),
            dma((2, n_col)),
            dma((n_col, 2, pieces)),
            dma,
            dma((tiles,)),
            dma((n_pair - 1,)),
            dma((n_pair - 1, tiles)),
            dma((n_col - 1,)),
            dma((n_col - 1,)),
            pltpu.SemaphoreType.REGULAR,
        ],
        compiler_params=pltpu.CompilerParams(
            collective_id=0, has_side_effects=True, vmem_limit_bytes=VMEM_BYTES
        ),
        name="down_reduce",
    )(gate_in, up_in, down_weight, residual, norm_gain.reshape(-1, 128))
    out = jax.ShapeDtypeStruct((half, local), jnp.bfloat16)
    return pl.pallas_call(
        finish, out_shape=(out, out), in_specs=[vmem] * 3, out_specs=(vmem, vmem), name="finish"
    )(total, pre, scale)


def pairs_share_chip(mesh):
    if tuple(mesh.axis_names) != ("tp", "col") or mesh.shape["tp"] % 2 or mesh.shape["tp"] < 4:
        return False
    devices = mesh.devices
    for j in range(0, mesh.shape["tp"], 2):
        for a, b in zip(devices[j], devices[j + 1]):
            first = getattr(a, "coords", None)
            if first is None or list(first) != list(getattr(b, "coords", ())):
                return False
    return True


def solution(mesh):
    in_specs = (P("col", "tp"), P("col", "tp"), P("tp", "col"), P("tp", "col"), P("col"))
    out_specs = (P("tp", "col"), P("tp", "col"))
    n_tp, n_col = mesh.shape["tp"], mesh.shape["col"]

    def run(gate_in, up_in, down_weight, residual, norm_gain):
        tokens, hidden_units = gate_in.shape
        width = down_weight.shape[1]
        depth, local = hidden_units // n_tp, width // n_col
        rows, own_rows = tokens // n_col, tokens // n_tp
        kp, nt, rt = pick(depth, 512, 128), pick(local, 1024, 128), pick(local, 512, 128)
        need = 2 * depth * (local + tokens + 2 * rows) + local * tokens * 9 + (4 << 20)
        fused = (
            pairs_share_chip(mesh)
            and n_col > 1
            and rows % 16 == 0
            and own_rows % 16 == 0
            and rows == 2 * own_rows
            and n_tp == 2 * n_col
            and local % 1024 == 0
            and kp > 0
            and SKEW < SPLIT + 1 < depth // kp
            and nt > 0
            and need < VMEM_BYTES
        )
        body = functools.partial(plain_body, width)
        if fused:
            body = functools.partial(fused_body, n_tp, n_col, kp, nt, rt, width)
        return jax.shard_map(
            body, mesh=mesh, in_specs=in_specs, out_specs=out_specs, check_vma=False
        )(gate_in, up_in, down_weight, residual, norm_gain)

    return run
```
